256 devices in a mesh: ha: 64 (over y_lo, z, x), ta: 4 (over y_hi, core).
Axes of the slice: x: 4, y: 4 (y_hi: 2, y_lo: 2; y = y_hi * 2 + y_lo), z: 8, core: 2. Of those that a mesh axis runs over, the one named last changes fastest.
Arguments:
- layer_input: bfloat16 [8, 192, 192, 128], P('ta', 'ha'), may hold values from -6 to 6
- pre_one: bfloat16 [8, 192, 192, 128], P('ta', 'ha'), may hold values from -9 to 9
- pre_two: bfloat16 [8, 192, 192, 128], P('ta', 'ha'), may hold values from -9 to 9
- pre_three: bfloat16 [8, 192, 192, 128], P('ta', 'ha'), may hold values from -9 to 9
- kernel_one: bfloat16 [3, 3, 3, 128, 128], replicated, may hold values from -0.109375 to 0.109375
- kernel_two: bfloat16 [3, 3, 3, 128, 128], replicated, may hold values from -0.109375 to 0.109375
- kernel_three: bfloat16 [3, 3, 3, 128, 128], replicated, may hold values from -0.109375 to 0.109375
- upstream: bfloat16 [8, 192, 192, 128], P('ta', 'ha'), may hold values from -24 to 24
Outputs:
- input_gradient: bfloat16 [8, 192, 192, 128], P('ta', 'ha')
- kernel_grad_one: float32 [3, 3, 3, 128, 128], P(None, None, None, 'ha')
- kernel_grad_two: float32 [3, 3, 3, 128, 128], P(None, None, None, 'ha')
- kernel_grad_three: float32 [3, 3, 3, 128, 128], P(None, None, None, 'ha')
The draws below stay inside these ranges and needn't reach their ends.
All inputs are finite; a program needn't handle non-finite values.
Results may differ from the reference program's by a relative error of at most 0.014.
Values may be sent and summed in bfloat16 or wider, within the bound.
No kernel may reach another device: no remote copies, remote signals or barrier semaphores. Data moves between devices by JAX's collectives and lax.ppermute only.
A program may use at most 128 MiB of HBM per device.

```python
import math
import jax
import jax.numpy as jnp
from jax import lax

C = 128
W = 192
F = 8
H = 192


def level_of(key, dims, cuts, smallest, largest):
    loudness = 1.0
    for position, shards_of in cuts:
        heights = jax.random.uniform(jax.random.fold_in(jax.random.fold_in(key, 6), position), (shards_of,), jnp.float32, smallest / len(cuts), largest / len(cuts))
        loudness = loudness * jnp.repeat(jnp.exp(heights), dims[position] // shards_of).reshape((-1,) + (1,) * (len(dims) - 1 - position))
    return loudness


def noise(key, shape, scale, reach, pieces=(), kind=jnp.bfloat16):
    result = scale * jax.random.normal(key, shape, jnp.float32)
    if pieces:
        result = result * level_of(key, shape, pieces, -0.22, 0.18)
    return jnp.clip(result, -reach, reach).astype(kind)


def setup_inputs(seed: int = 0) -> dict:
    streams_of = jax.random.split(jax.random.key(seed), 9)
    layer_input = noise(streams_of[0], (F, H, W, C), 1.0, 6.0, ((0, 4), (1, 64)))
    pre_one = noise(streams_of[1], (F, H, W, C), 1.5, 9.0, ((0, 4), (1, 64)))
    pre_two = noise(streams_of[2], (F, H, W, C), 1.5, 9.0, ((0, 4), (1, 64)))
    pre_three = noise(streams_of[3], (F, H, W, C), 1.5, 9.0, ((0, 4), (1, 64)))
    kernel_one = noise(streams_of[4], (3, 3, 3, C, C), (27 * C) ** -0.5, 0.109375)
    kernel_two = noise(streams_of[5], (3, 3, 3, C, C), (27 * C) ** -0.5, 0.109375)
    kernel_three = noise(streams_of[6], (3, 3, 3, C, C), (27 * C) ** -0.5, 0.109375)
    upstream = noise(streams_of[7], (F, H, W, C), 4.0, 24.0, ((0, 4), (1, 64)))
    return {"layer_input": layer_input, "pre_one": pre_one, "pre_two": pre_two, "pre_three": pre_three, "kernel_one": kernel_one, "kernel_two": kernel_two, "kernel_three": kernel_three, "upstream": upstream}


def silu_slope(pre_values):
    values = pre_values.astype(jnp.float32)
    sigmoid = jax.nn.sigmoid(values)
    return sigmoid * (1.0 + values * (1.0 - sigmoid))

def kernel_grad(inputs, gradient):
    padded = jnp.pad(inputs, ((2, 0), (1, 1), (1, 1), (0, 0)))
    norm_scale = 1.0 / math.sqrt(F * H * W)

    def step(running, frame_index):
        window = lax.dynamic_slice_in_dim(padded, frame_index, 3, 0)
        tap_list = [window[tap_time, tap_row:tap_row + H, tap_col:tap_col + W] for tap_time in range(3) for tap_row in range(3) for tap_col in range(3)]
        patches = jnp.concatenate(tap_list, -1).reshape(H * W, 27 * C)
        current = lax.dynamic_index_in_dim(gradient, frame_index, 0, keepdims=False).reshape(H * W, C)
        contribution = lax.dot_general(patches, current, (((0,), (0,)), ((), ())), preferred_element_type=jnp.float32)
        return (running + contribution, None)
    running, _ = lax.scan(step, jnp.zeros((27 * C, C), jnp.float32), jnp.arange(F, dtype=jnp.int32))
    return (running * norm_scale).reshape(3, 3, 3, C, C)

def input_grad(gradient, kernel):
    padded = jnp.pad(gradient, ((0, 2), (1, 1), (1, 1), (0, 0)))
    flipped = jnp.swapaxes(kernel, 3, 4).reshape(27 * C, C)

    def frame_result(frame_index):
        window = lax.dynamic_slice_in_dim(padded, frame_index, 3, 0)
        tap_list = [window[2 - tap_time, 2 - tap_row:2 - tap_row + H, 2 - tap_col:2 - tap_col + W] for tap_time in range(3) for tap_row in range(3) for tap_col in range(3)]
        patches = jnp.concatenate(tap_list, -1).reshape(H * W, 27 * C)
        return jnp.dot(patches, flipped, preferred_element_type=jnp.float32)
    return lax.map(frame_result, jnp.arange(F, dtype=jnp.int32)).reshape(F, H, W, C)

def reference(layer_input, pre_one, pre_two, pre_three, kernel_one, kernel_two, kernel_three, upstream):
    act_one = jax.nn.silu(pre_one.astype(jnp.float32)).astype(jnp.bfloat16)
    act_two = jax.nn.silu(pre_two.astype(jnp.float32)).astype(jnp.bfloat16)
    grad_three = (upstream.astype(jnp.float32) * silu_slope(pre_three)).astype(jnp.bfloat16)
    kernel_grad_three = kernel_grad(act_two, grad_three)
    grad_two = (input_grad(grad_three, kernel_three) * silu_slope(pre_two)).astype(jnp.bfloat16)
    kernel_grad_two = kernel_grad(act_one, grad_two)
    grad_one = (input_grad(grad_two, kernel_two) * silu_slope(pre_one)).astype(jnp.bfloat16)
    kernel_grad_one = kernel_grad(layer_input, grad_one)
    input_gradient = input_grad(grad_one, kernel_one).astype(jnp.bfloat16)
    return (input_gradient, kernel_grad_one, kernel_grad_two, kernel_grad_three)
```

```python
import functools
import math

import jax
import jax.numpy as jnp
from jax import lax
from jax.experimental import pallas as pl
from jax.experimental.pallas import tpu as pltpu
from jax.sharding import PartitionSpec as P


HALO = 8
OUTSIDE = -1000.0
TAPS = 27
SLOTS = 32
MIB = 1024 * 1024
LIMIT = 18
VMEM = pl.BlockSpec(memory_space=pltpu.VMEM)
SMEM = pl.BlockSpec(memory_space=pltpu.SMEM)
GROUPS = ((0, 1), (2, 3), (4, 5), (6, 7), (8,))


def call(body, out_shape, operands, flops, scratch=(), scalar=None):
    moved = sum(a.size * a.dtype.itemsize for a in operands)
    moved += sum(math.prod(s.shape) * s.dtype.itemsize for s in out_shape)
    count, results = len(operands), len(out_shape)
    skip = 0 if scalar is None else 1

    def kernel(*refs):
        loaded = refs[skip : skip + count]
        rest = refs[skip + count :]
        body(*refs[:skip], loaded, rest[:results], *rest[results:])

    return pl.pallas_call(
        kernel,
        out_shape=tuple(out_shape),
        in_specs=[SMEM] * skip + [VMEM] * count,
        out_specs=(VMEM,) * results,
        scratch_shapes=list(scratch),
        compiler_params=pltpu.CompilerParams(vmem_limit_bytes=LIMIT * MIB),
        cost_estimate=pl.CostEstimate(flops=flops, bytes_accessed=moved, transcendentals=0),
    )(*([] if scalar is None else [scalar]), *operands)


def slope(pre_values):
    values = pre_values.astype(jnp.float32)
    sigmoid = jax.nn.sigmoid(values)
    return sigmoid * (1.0 + values * (1.0 - sigmoid))


def silu(pre_values):
    values = pre_values.astype(jnp.float32)
    return (values * jax.nn.sigmoid(values)).astype(jnp.bfloat16)


def split_columns(value, out_ref, outside):
    parts, own = out_ref.shape[0], out_ref.shape[3] - 2 * HALO
    shape = value.shape[:2] + (2 * HALO, value.shape[3])
    fill = jnp.full(shape, outside, value.dtype)
    first = lax.broadcasted_iota(jnp.int32, shape, 2) < HALO
    for part in range(parts):
        begin, end = part * own, (part + 1) * own
        out_ref[part, :, :, 0:own] = value[:, :, begin:end]
        right = value[:, :, end : end + 2 * HALO] if part < parts - 1 else fill
        left = value[:, :, begin - 2 * HALO : begin] if part else fill
        tail = jnp.where(first, right.astype(jnp.float32), left.astype(jnp.float32))
        out_ref[part, :, :, own : own + 2 * HALO] = tail.astype(value.dtype)


def split_first(loaded, outs):
    upstream, pre, two = loaded
    (out_ref,) = outs
    wide = out_ref.shape[3] // 2
    upstream_ref, pre_ref = upstream, pre
    gradient = upstream_ref[...].astype(jnp.float32) * slope(pre_ref[...])
    split_columns(gradient.astype(jnp.bfloat16), out_ref.at[:, :, :, 0:wide], 0.0)
    split_columns(two[...], out_ref.at[:, :, :, wide : 2 * wide], OUTSIDE)


def split_second(loaded, outs):
    (out_ref,) = outs
    one_ref, input_ref = loaded[0], loaded[1]
    parts = out_ref.shape[0]
    own = input_ref.shape[2] // parts
    wide = own + 2 * HALO
    split_columns(one_ref[...], out_ref.at[:, :, :, 0:wide], OUTSIDE)
    for part in range(parts):
        out_ref[part, :, :, wide : wide + own] = input_ref[:, :, part * own : (part + 1) * own]


def fill_window(own, before, after, window_ref):
    own_ref, before_ref, after_ref = own, before, after
    frames, rows, channels = own_ref.shape[0], own_ref.shape[1], own_ref.shape[3]
    cols = before_ref.shape[1]
    window_ref[frames : frames + 2] = jnp.zeros((2,) + window_ref.shape[1:], window_ref.dtype)
    for frame in range(frames):
        sources = [before_ref[frame]] + [own_ref[frame, r, 0:cols] for r in range(rows)] + [after_ref[frame]]
        for r, block in enumerate(sources):
            wide = block.astype(jnp.float32)
            following = pltpu.roll(wide, cols - 1, 0).astype(window_ref.dtype)
            preceding = pltpu.roll(wide, 1, 0).astype(window_ref.dtype)
            window_ref[frame, r, :, 0:channels] = following
            window_ref[frame, r, :, channels : 2 * channels] = block
            window_ref[frame, r, :, 2 * channels : 3 * channels] = preceding


def input_grad_kernel(loaded, outs, window_ref, *, begin):
    own, before, after, kernel, *pre = loaded
    frames, rows, channels = own.shape[0], own.shape[1], own.shape[3]
    cols = before.shape[1]
    out_ref, width = outs[0], outs[0].shape[2]
    fill_window(own, before, after, window_ref)
    kernel_ref = kernel
    if pre:
        pre_ref = pre[0]
        first_ref, final_ref = outs[1:]
    weights = []
    for group in GROUPS:
        weights.append(
            jnp.concatenate([kernel_ref[3 * pair + c] for pair in group for c in range(3)], -1)
        )
    step = 2
    for f in range(0, frames, step):
        total = None
        for group, weight in zip(GROUPS, weights):
            pieces = []
            for pair in group:
                a, b = divmod(pair, 3)
                block = window_ref[f + 2 - a : f + 2 - a + step, 2 - b : 2 - b + rows, 0:width]
                pieces.append(block.reshape(step * rows * width, 3 * channels))
            patches = jnp.concatenate(pieces, -1) if len(pieces) > 1 else pieces[0]
            term = lax.dot_general(
                patches, weight, (((1,), (1,)), ((), ())), preferred_element_type=jnp.float32
            )
            total = term if total is None else total + term
        total = total.reshape(step, rows, width, channels)
        if not pre:
            out_ref[f : f + step] = total.astype(jnp.bfloat16)
        else:
            result = (total * slope(pre_ref[f : f + step, :, begin : begin + cols])).astype(jnp.bfloat16)
            out_ref[f : f + step] = result
            first_ref[f : f + step] = result[:, 0]
            final_ref[f : f + step] = result[:, rows - 1]


def kernel_grad_kernel(half_ref, loaded, outs, window_ref, spread_ref, *, activate, width, begin):
    own, before, after, kept = loaded
    keep_ref, send_ref = outs
    frames, rows, channels = own.shape[0], own.shape[1], own.shape[3]
    cells = frames * rows * width
    half = channels // 2
    fill_window(own, before, after, window_ref)
    saved = kept[:, :, begin : begin + width]
    if activate:
        saved = silu(saved)
    left = saved.reshape(cells, channels).T
    spread_ref[...] = jnp.zeros(spread_ref.shape, spread_ref.dtype)
    for pair in range(9):
        a, b = divmod(pair, 3)
        block = window_ref[2 - a : 2 - a + frames, 2 - b : 2 - b + rows, 0:width]
        term = jnp.dot(
            left, block.reshape(cells, 3 * channels), preferred_element_type=jnp.float32
        )
        for c in range(3):
            spread_ref[pl.ds(3 * pair + c, channels, stride=SLOTS), :] = term[
                :, c * channels : (c + 1) * channels
            ]
    paired = spread_ref.reshape(half, 2 * SLOTS, channels)
    mine = pl.multiple_of(half_ref[0] * SLOTS, SLOTS)
    other = pl.multiple_of((1 - half_ref[0]) * SLOTS, SLOTS)
    keep_ref[...] = paired[:, pl.ds(mine, SLOTS), :]
    send_ref[...] = paired[:, pl.ds(other, SLOTS), :].astype(jnp.bfloat16)


def window_scratch(own, cols):
    frames, rows, _, channels = own.shape
    return pltpu.VMEM((frames + 2, rows + 2, cols, 3 * channels), jnp.bfloat16)


def input_grad(own, before, after, kernel, pre, width, begin):
    frames, rows, _, channels = own.shape
    cols = before.shape[1]
    flops = 2 * TAPS * frames * rows * cols * channels * channels
    taps = kernel.reshape(TAPS, channels, channels)
    if pre is None:
        shape = jax.ShapeDtypeStruct((frames, rows, width, channels), jnp.bfloat16)
        outs, operands = (shape,), (own, before, after, taps)
    else:
        shape = jax.ShapeDtypeStruct((frames, rows, cols, channels), jnp.bfloat16)
        edge = jax.ShapeDtypeStruct((frames, cols, channels), jnp.bfloat16)
        outs, operands = (shape, edge, edge), (own, before, after, taps, pre)
    body = functools.partial(input_grad_kernel, begin=begin)
    scratch = [window_scratch(own, cols)]
    return call(body, outs, operands, flops, scratch)


def kernel_grad(half, own, before, after, saved, activate, width, begin):
    frames, rows, _, channels = own.shape
    cols = before.shape[1]
    flops = 2 * TAPS * frames * rows * width * channels * channels
    shape = (channels // 2, SLOTS, channels)
    outs = (jax.ShapeDtypeStruct(shape, jnp.float32), jax.ShapeDtypeStruct(shape, jnp.bfloat16))
    body = functools.partial(kernel_grad_kernel, activate=activate, width=width, begin=begin)
    scratch = [
        window_scratch(own, cols),
        pltpu.VMEM((channels * SLOTS, channels), jnp.float32),
    ]
    return call(body, outs, (own, before, after, saved), flops, scratch, scalar=half)


def swapped(x, bit):
    return lax.ppermute(x, "ta", [(i, i ^ bit) for i in range(lax.axis_size("ta"))])


def row_halo(first, final):
    peers = lax.axis_size("ha")
    before = lax.ppermute(final, "ha", [(i, i + 1) for i in range(peers - 1)])
    after = lax.ppermute(first, "ha", [(i + 1, i) for i in range(peers - 1)])
    return before, after


def across(x):
    return lax.all_to_all(x, "ta", 0, 0, tiled=True)


def returned(blocks):
    parts = blocks.shape[0]
    me = lax.axis_index("ta")
    pieces = [lax.dynamic_index_in_dim(blocks, me, 0, False)]
    for bits in range(1, parts):
        pieces.append(swapped(lax.dynamic_index_in_dim(blocks, me ^ bits, 0, False), bits))
    stacked = jnp.stack(pieces)
    ordered = [lax.dynamic_index_in_dim(stacked, me ^ part, 0, False) for part in range(parts)]
    return jnp.concatenate(ordered, 2)


def fold_rows(joined, upper):
    peers = lax.axis_size("ha")
    size = peers // 2
    send = lax.dynamic_slice_in_dim(joined, (1 - upper) * size, size, 0)
    keep = lax.dynamic_slice_in_dim(joined, upper * size, size, 0)
    other = lax.ppermute(send, "ha", [(i, (i + size) % peers) for i in range(peers)])
    total = keep.astype(jnp.float32) + other.astype(jnp.float32)
    return total.astype(jnp.bfloat16)


def shards(
    layer_input, pre_one, pre_two, pre_three, kernel_one, kernel_two, kernel_three, upstream
):
    frames, rows, columns, channels = layer_input.shape
    parts = lax.axis_size("ta")
    width = columns // parts
    cells_total = layer_input.size // channels * parts * lax.axis_size("ha")
    norm_scale = 1.0 / math.sqrt(cells_total)
    half = (lax.axis_index("ta") % 2).astype(jnp.int32)
    upper = (lax.axis_index("ha") // (lax.axis_size("ha") // 2)).astype(jnp.int32)
    wide = width + 2 * HALO
    first_shape = jax.ShapeDtypeStruct((parts, frames, rows, 2 * wide, channels), jnp.bfloat16)
    second_shape = (parts, frames, rows, wide + width, channels)
    second_shape = jax.ShapeDtypeStruct(second_shape, jnp.bfloat16)

    def gathered(block):
        moved = across(block)
        return moved.reshape((parts * frames,) + moved.shape[2:])

    block = call(split_first, (first_shape,), (upstream, pre_three, pre_two), 10**6)[0]
    grad = gathered(block)
    block = call(split_second, (second_shape,), (pre_one, layer_input), 10**6)[0]
    before, after = row_halo(grad[:, 0, 0:wide], grad[:, rows - 1, 0:wide])
    second = gathered(block)

    def kernel_term(saved, activate, begin):
        keep, send = kernel_grad(
            half.reshape(1), grad, before, after, saved, activate, width, begin
        )
        return keep + swapped(send, 1).astype(jnp.float32)

    saved = grad
    outs = input_grad(grad, before, after, kernel_three, saved, width, wide)
    term_three = kernel_term(saved, True, wide).astype(jnp.bfloat16)
    term_three = fold_rows(term_three, upper)
    grad = outs[0]
    before, after = row_halo(outs[1], outs[2])
    outs = input_grad(grad, before, after, kernel_two, second, width, 0)
    term_two = kernel_term(second, True, 0).astype(jnp.bfloat16)
    term_two = fold_rows(term_two, upper)
    grad = outs[0]
    before, after = row_halo(outs[1], outs[2])
    late = kernel_term(second, False, wide).astype(jnp.bfloat16)
    late = fold_rows(late, upper)
    size = lax.axis_size("ha") // 2
    halves = [[start + i for i in range(size)] for start in (0, size)]
    terms = lax.all_to_all(
        jnp.concatenate([term_three, term_two, late], 1), "ha", 0, 0, axis_index_groups=halves, tiled=True
    )
    own = input_grad(grad, before, after, kernel_one, None, width, 0)[0]
    back = returned(own.reshape((parts, frames) + own.shape[1:]))
    back = back.reshape(layer_input.shape)
    mine = jnp.sum(terms.astype(jnp.float32), 0).reshape(3, SLOTS, channels)
    mine = mine + swapped(mine, 2)
    theirs = swapped(mine, 1)
    low = jnp.where(half == 0, mine, theirs)
    high = jnp.where(half == 0, theirs, mine)
    both = jnp.stack([low, high], 2)[:, :TAPS] * norm_scale
    grads = [both[layer].reshape(3, 3, 3, 2, channels) for layer in range(3)]
    return (back, grads[2], grads[1], grads[0])


def solution(mesh):
    cells = P("ta", "ha", None, None)
    grads = P(None, None, None, "ha", None)
    return jax.shard_map(
        shards,
        mesh=mesh,
        in_specs=(cells, cells, cells, cells, P(), P(), P(), cells),
        out_specs=(cells, grads, grads, grads),
        check_vma=False,
    )
```

```python
import functools
import math

import jax
import jax.numpy as jnp
from jax import lax
from jax.experimental import pallas as pl
from jax.experimental.pallas import tpu as pltpu
from jax.sharding import PartitionSpec as P


HALO = 8
OUTSIDE = -1000.0
TAPS = 27
SLOTS = 32
MIB = 1024 * 1024
LIMIT = 18
VMEM = pl.BlockSpec(memory_space=pltpu.VMEM)
HBM = pl.BlockSpec(memory_space=pltpu.HBM)
SMEM = pl.BlockSpec(memory_space=pltpu.SMEM)
GROUPS = ((0, 1), (2, 3), (4, 5), (6, 7), (8,))


def call(body, out_shape, operands, flops, scratch=(), scalar=None, fetched=False):
    moved = sum(a.size * a.dtype.itemsize for a in operands)
    moved += sum(math.prod(s.shape) * s.dtype.itemsize for s in out_shape)
    count, results = len(operands), len(out_shape)
    skip = 0 if scalar is None else 1
    local = []
    if fetched:
        local = [pltpu.VMEM(a.shape, a.dtype) for a in operands]
        local.append(pltpu.SemaphoreType.DMA((count,)))

    def kernel(*refs):
        loaded = refs[skip : skip + count]
        rest = refs[skip + count :]
        if fetched:
            semaphores = rest[-1]
            sources, loaded, rest = loaded, rest[-1 - count : -1], rest[: -1 - count]
            copies = [
                pltpu.make_async_copy(source, local, semaphores.at[i])
                for i, (source, local) in enumerate(zip(sources, loaded))
            ]
            for copy in copies:
                copy.start()
            for copy in copies:
                copy.wait()
        body(*refs[:skip], loaded, rest[:results], *rest[results:])

    return pl.pallas_call(
        kernel,
        out_shape=tuple(out_shape),
        in_specs=[SMEM] * skip + [HBM if fetched else VMEM] * count,
        out_specs=(VMEM,) * results,
        scratch_shapes=list(scratch) + local,
        compiler_params=pltpu.CompilerParams(vmem_limit_bytes=(60 if fetched else LIMIT) * MIB),
        cost_estimate=pl.CostEstimate(flops=flops, bytes_accessed=moved, transcendentals=0),
    )(*([] if scalar is None else [scalar]), *operands)


def slope(pre_values):
    values = pre_values.astype(jnp.float32)
    sigmoid = jax.nn.sigmoid(values)
    return sigmoid * (1.0 + values * (1.0 - sigmoid))


def silu(pre_values):
    values = pre_values.astype(jnp.float32)
    return (values * jax.nn.sigmoid(values)).astype(jnp.bfloat16)


def split_columns(value, out_ref, outside):
    parts, own = out_ref.shape[0], out_ref.shape[3] - 2 * HALO
    shape = value.shape[:2] + (2 * HALO, value.shape[3])
    fill = jnp.full(shape, outside, value.dtype)
    first = lax.broadcasted_iota(jnp.int32, shape, 2) < HALO
    for part in range(parts):
        begin, end = part * own, (part + 1) * own
        out_ref[part, :, :, 0:own] = value[:, :, begin:end]
        right = value[:, :, end : end + 2 * HALO] if part < parts - 1 else fill
        left = value[:, :, begin - 2 * HALO : begin] if part else fill
        tail = jnp.where(first, right.astype(jnp.float32), left.astype(jnp.float32))
        out_ref[part, :, :, own : own + 2 * HALO] = tail.astype(value.dtype)


def split_first(loaded, outs):
    upstream, pre, two = loaded
    (out_ref,) = outs
    wide = out_ref.shape[3] // 2
    upstream_ref, pre_ref = upstream, pre
    gradient = upstream_ref[...].astype(jnp.float32) * slope(pre_ref[...])
    split_columns(gradient.astype(jnp.bfloat16), out_ref.at[:, :, :, 0:wide], 0.0)
    split_columns(two[...], out_ref.at[:, :, :, wide : 2 * wide], OUTSIDE)


def split_second(place_ref, loaded, outs, block_ref):
    one_ref, input_ref = loaded
    parts = len(outs)
    own = input_ref.shape[2] // parts
    wide = own + 2 * HALO
    split_columns(one_ref[...], block_ref.at[:, :, :, 0:wide], OUTSIDE)
    for part in range(parts):
        block_ref[part, :, :, wide : wide + own] = input_ref[:, :, part * own : (part + 1) * own]
    for bits, out_ref in enumerate(outs):
        out_ref[...] = block_ref[place_ref[2] ^ bits]


def in_order(place_ref, pieces, whole_ref):
    frames = pieces[0].shape[0]
    if len(pieces) == 1:
        return pieces[0]
    for bits, piece in enumerate(pieces):
        whole_ref[pl.ds((place_ref[2] ^ bits) * frames, frames)] = piece[...]
    return whole_ref


def fill_window(own, before, after, window_ref):
    own_ref, before_ref, after_ref = own, before, after
    frames, rows, channels = own_ref.shape[0], own_ref.shape[1], own_ref.shape[3]
    cols = before_ref.shape[1]
    window_ref[frames : frames + 2] = jnp.zeros((2,) + window_ref.shape[1:], window_ref.dtype)
    for frame in range(frames):
        sources = [before_ref[frame]] + [own_ref[frame, r, 0:cols] for r in range(rows)] + [after_ref[frame]]
        for r, block in enumerate(sources):
            wide = block.astype(jnp.float32)
            following = pltpu.roll(wide, cols - 1, 0).astype(window_ref.dtype)
            preceding = pltpu.roll(wide, 1, 0).astype(window_ref.dtype)
            window_ref[frame, r, :, 0:channels] = following
            window_ref[frame, r, :, channels : 2 * channels] = block
            window_ref[frame, r, :, 2 * channels : 3 * channels] = preceding


def input_grad_kernel(place_ref, loaded, outs, window_ref, *whole_ref, begin):
    own, before, after, kernel, *pre = loaded
    frames, rows, channels = own.shape[0], own.shape[1], own.shape[3]
    cols = before.shape[1]
    out_ref, width = outs[0], outs[0].shape[2]
    fill_window(own, before, after, window_ref)
    kernel_ref = kernel
    if pre:
        pre_ref = in_order(place_ref, pre, *whole_ref) if whole_ref else pre[0]
        first_ref, final_ref = outs[1:]
    weights = []
    for group in GROUPS:
        weights.append(
            jnp.concatenate([kernel_ref[3 * pair + c] for pair in group for c in range(3)], -1)
        )
    step = 2
    for f in range(0, frames, step):
        total = None
        for group, weight in zip(GROUPS, weights):
            pieces = []
            for pair in group:
                a, b = divmod(pair, 3)
                block = window_ref[f + 2 - a : f + 2 - a + step, 2 - b : 2 - b + rows, 0:width]
                pieces.append(block.reshape(step * rows * width, 3 * channels))
            patches = jnp.concatenate(pieces, -1) if len(pieces) > 1 else pieces[0]
            term = lax.dot_general(
                patches, weight, (((1,), (1,)), ((), ())), preferred_element_type=jnp.float32
            )
            total = term if total is None else total + term
        total = total.reshape(step, rows, width, channels)
        if not pre:
            out_ref[f : f + step] = total.astype(jnp.bfloat16)
        else:
            result = (total * slope(pre_ref[f : f + step, :, begin : begin + cols])).astype(jnp.bfloat16)
            out_ref[f : f + step] = result
            first_ref[f : f + step] = result[:, 0]
            final_ref[f : f + step] = result[:, rows - 1]


def kernel_grad_kernel(
    place_ref, loaded, outs, window_ref, spread_ref, *whole_ref, activate, width, begin
):
    own, before, after, *kept = loaded
    keep_ref, send_ref = outs
    frames, rows, channels = own.shape[0], own.shape[1], own.shape[3]
    cells = frames * rows * width
    half = channels // 2
    fill_window(own, before, after, window_ref)
    kept_ref = in_order(place_ref, kept, *whole_ref) if whole_ref else kept[0]
    saved = kept_ref[:, :, begin : begin + width]
    if activate:
        saved = silu(saved)
    left = saved.reshape(cells, channels).T
    spread_ref[...] = jnp.zeros(spread_ref.shape, spread_ref.dtype)
    for pair in range(9):
        a, b = divmod(pair, 3)
        block = window_ref[2 - a : 2 - a + frames, 2 - b : 2 - b + rows, 0:width]
        term = jnp.dot(
            left, block.reshape(cells, 3 * channels), preferred_element_type=jnp.float32
        )
        for c in range(3):
            spread_ref[pl.ds(3 * pair + c, channels, stride=SLOTS), :] = term[
                :, c * channels : (c + 1) * channels
            ]
    paired = spread_ref.reshape(half, 2 * SLOTS, channels)
    mine = pl.multiple_of(place_ref[0] * SLOTS, SLOTS)
    other = pl.multiple_of((1 - place_ref[0]) * SLOTS, SLOTS)
    size = half // 2
    for place, begin_row in enumerate(((1 - place_ref[1]) * size, place_ref[1] * size)):
        span = pl.ds(begin_row, size)
        keep_ref[place] = paired[span, pl.ds(mine, SLOTS), :]
        send_ref[place] = paired[span, pl.ds(other, SLOTS), :].astype(jnp.bfloat16)


def window_scratch(own, cols):
    frames, rows, _, channels = own.shape
    return pltpu.VMEM((frames + 2, rows + 2, cols, 3 * channels), jnp.bfloat16)


def whole_scratch(pieces):
    if len(pieces) == 1:
        return []
    shape = (len(pieces) * pieces[0].shape[0],) + pieces[0].shape[1:]
    return [pltpu.VMEM(shape, pieces[0].dtype)]


def input_grad(place, own, before, after, kernel, pre, width, begin):
    frames, rows, _, channels = own.shape
    cols = before.shape[1]
    flops = 2 * TAPS * frames * rows * cols * channels * channels
    taps = kernel.reshape(TAPS, channels, channels)
    if pre is None:
        shape = jax.ShapeDtypeStruct((frames, rows, width, channels), jnp.bfloat16)
        outs, operands = (shape,), (own, before, after, taps)
    else:
        shape = jax.ShapeDtypeStruct((frames, rows, cols, channels), jnp.bfloat16)
        edge = jax.ShapeDtypeStruct((frames, cols, channels), jnp.bfloat16)
        outs, operands = (shape, edge, edge), (own, before, after, taps, *pre)
    body = functools.partial(input_grad_kernel, begin=begin)
    scratch = [window_scratch(own, cols)] + (whole_scratch(pre) if pre else [])
    return call(body, outs, operands, flops, scratch, place)


def kernel_grad(place, own, before, after, saved, activate, width, begin):
    frames, rows, _, channels = own.shape
    cols = before.shape[1]
    flops = 2 * TAPS * frames * rows * width * channels * channels
    shape = (2, channels // 4, SLOTS, channels)
    outs = (jax.ShapeDtypeStruct(shape, jnp.float32), jax.ShapeDtypeStruct(shape, jnp.bfloat16))
    body = functools.partial(kernel_grad_kernel, activate=activate, width=width, begin=begin)
    scratch = [
        window_scratch(own, cols),
        pltpu.VMEM((channels * SLOTS, channels), jnp.float32),
    ]
    scratch += whole_scratch(saved)
    return call(body, outs, (own, before, after, *saved), flops, scratch, place)


def swapped(x, bit):
    return lax.ppermute(x, "ta", [(i, i ^ bit) for i in range(lax.axis_size("ta"))])


def row_halo(first, final):
    peers = lax.axis_size("ha")
    before = lax.ppermute(final, "ha", [(i, i + 1) for i in range(peers - 1)])
    after = lax.ppermute(first, "ha", [(i + 1, i) for i in range(peers - 1)])
    return before, after


def across(x):
    return lax.all_to_all(x, "ta", 0, 0, tiled=True)


def returned(blocks):
    parts = blocks.shape[0]
    me = lax.axis_index("ta")
    pieces = [lax.dynamic_index_in_dim(blocks, me, 0, False)]
    for bits in range(1, parts):
        pieces.append(swapped(lax.dynamic_index_in_dim(blocks, me ^ bits, 0, False), bits))
    stacked = jnp.stack(pieces)
    ordered = [lax.dynamic_index_in_dim(stacked, me ^ part, 0, False) for part in range(parts)]
    return jnp.concatenate(ordered, 2)


def fold_rows(keep, received):
    peers = lax.axis_size("ha")
    size = peers // 2
    send = (keep[0] + received[0].astype(jnp.float32)).astype(jnp.bfloat16)
    other = lax.ppermute(send, "ha", [(i, (i + size) % peers) for i in range(peers)])
    total = keep[1] + received[1].astype(jnp.float32) + other.astype(jnp.float32)
    return total.astype(jnp.bfloat16)


def shards(
    layer_input, pre_one, pre_two, pre_three, kernel_one, kernel_two, kernel_three, upstream
):
    frames, rows, columns, channels = layer_input.shape
    parts = lax.axis_size("ta")
    width = columns // parts
    cells_total = layer_input.size // channels * parts * lax.axis_size("ha")
    norm_scale = 1.0 / math.sqrt(cells_total)
    half = (lax.axis_index("ta") % 2).astype(jnp.int32)
    upper = (lax.axis_index("ha") // (lax.axis_size("ha") // 2)).astype(jnp.int32)
    wide = width + 2 * HALO
    first_shape = jax.ShapeDtypeStruct((parts, frames, rows, 2 * wide, channels), jnp.bfloat16)
    second_shape = (frames, rows, wide + width, channels)
    second_shapes = (jax.ShapeDtypeStruct(second_shape, jnp.bfloat16),) * parts
    block_scratch = pltpu.VMEM((parts,) + second_shape, jnp.bfloat16)
    place = jnp.stack([half, upper, lax.axis_index("ta").astype(jnp.int32)])

    def gathered(block):
        moved = across(block)
        return moved.reshape((parts * frames,) + moved.shape[2:])

    operands = (upstream, pre_three, pre_two)
    block = call(split_first, (first_shape,), operands, 10**6, fetched=True)[0]
    grad = gathered(block)
    operands = (pre_one, layer_input)
    blocks = call(split_second, second_shapes, operands, 10**6, [block_scratch], place)
    before, after = row_halo(grad[:, 0, 0:wide], grad[:, rows - 1, 0:wide])
    second = [blocks[0]] + [swapped(blocks[bits], bits) for bits in range(1, parts)]

    def kernel_term(saved, activate, begin):
        keep, send = kernel_grad(
            place, grad, before, after, saved, activate, width, begin
        )
        return keep, swapped(send, 1)

    saved = [grad]
    outs = input_grad(place, grad, before, after, kernel_three, saved, width, wide)
    term_three = kernel_term(saved, True, wide)
    term_three = fold_rows(*term_three)
    grad = outs[0]
    before, after = row_halo(outs[1], outs[2])
    outs = input_grad(place, grad, before, after, kernel_two, second, width, 0)
    term_two = kernel_term(second, True, 0)
    term_two = fold_rows(*term_two)
    grad = outs[0]
    before, after = row_halo(outs[1], outs[2])
    late = kernel_term(second, False, wide)
    late = fold_rows(*late)
    size = lax.axis_size("ha") // 2
    halves = [[start + i for i in range(size)] for start in (0, size)]
    terms = lax.all_to_all(
        jnp.concatenate([term_three, term_two, late], 1), "ha", 0, 0, axis_index_groups=halves, tiled=True
    )
    own = input_grad(place, grad, before, after, kernel_one, None, width, 0)[0]
    back = returned(own.reshape((parts, frames) + own.shape[1:]))
    back = back.reshape(layer_input.shape)
    mine = jnp.sum(terms.astype(jnp.float32), 0).reshape(3, SLOTS, channels)
    far, across_far, near = swapped(mine, 2), swapped(mine, 3), swapped(mine, 1)
    mine, theirs = mine + far, near + across_far
    low = jnp.where(half == 0, mine, theirs)
    high = jnp.where(half == 0, theirs, mine)
    both = jnp.stack([low, high], 2)[:, :TAPS] * norm_scale
    grads = [both[layer].reshape(3, 3, 3, 2, channels) for layer in range(3)]
    return (back, grads[2], grads[1], grads[0])


def solution(mesh):
    cells = P("ta", "ha", None, None)
    grads = P(None, None, None, "ha", None)
    return jax.shard_map(
        shards,
        mesh=mesh,
        in_specs=(cells, cells, cells, cells, P(), P(), P(), cells),
        out_specs=(cells, grads, grads, grads),
        check_vma=False,
    )
```
